32 devices in a mesh: blk: 4 (over y, x), head: 8 (over z, core).
Axes of the slice: x: 2, y: 2, z: 4, core: 2. Of those that a mesh axis runs over, the one named last changes fastest.
Arguments:
- queries: bfloat16 [2048, 12288], P(('blk', 'head')), may hold values from -64 to 64, as said below
- exponents: int32 [2048, 64], P(('blk', 'head')), may hold values from -2 to 2
- latent: bfloat16 [2048, 576], P(('blk', 'head')), may hold values from -6 to 6, as said below
- segments: int32 [2048], P(('blk', 'head')), may hold values from 0 to 11, never falling along the last dimension, each value on 1 to 256 neighbouring positions
- key_weight: bfloat16 [512, 8192], P(None, 'head'), may hold values from -0.25 to 0.25
- value_weight: bfloat16 [512, 8192], P(None, 'head'), may hold values from -0.25 to 0.25
Outputs:
- attended: bfloat16 [2048, 8192], P(('blk', 'head'))
The draws below stay inside these ranges and needn't reach their ends.
Inputs may be any that keep to these rules, and one draw needn't show every extreme that they name: queries stay within the range. `latent`: latents stay within the range. `segments`: document numbers never fall along the sequence, and a document holds at most 256 tokens.
All inputs are finite; a program needn't handle non-finite values.
Results may differ from the reference program's by a relative error of at most 0.0069.
Values may be sent and summed in bfloat16 or wider, within the bound.
No kernel may reach another device: no remote copies, remote signals or barrier semaphores. Data moves between devices by JAX's collectives and lax.ppermute only.
A program may use at most 64 MiB of HBM per device.

```python
import math
import jax
import jax.numpy as jnp
import numpy as np
from jax import lax

HEADS = 64
NOPE = 128
ROPE = 64
LATENT = 512
VDIM = 128
TOKENS = 2048
MOST = 256
BLOCK = 512
LEAD = 512
N_BLK = 4


def latent_base(key):
    return jnp.clip(jax.random.normal(jax.random.fold_in(key, 11), (TOKENS, LATENT + ROPE), jnp.float32), -6.0, 6.0)


def draw_latent(key, part):
    return latent_base(key).astype(jnp.bfloat16)


def draw_queries(key, part):
    base = jax.random.normal(jax.random.fold_in(key, 23), (TOKENS, HEADS, NOPE + ROPE), jnp.float32)
    base = jnp.clip(base, -6.0, 6.0)
    return base.reshape(TOKENS, HEADS * (NOPE + ROPE)).astype(jnp.bfloat16)


def touch_ends(drawn, rng, low, high):
    longest = drawn.shape.index(max(drawn.shape))
    spots = []
    for shift in (0, 1):
        where = [jax.random.randint(jax.random.fold_in(rng, axis), (), 0, length) for axis, length in enumerate(drawn.shape)]
        where[longest] = (where[longest] + shift) % drawn.shape[longest]
        spots.append(tuple(where))
    return drawn.at[spots[0]].set(low).at[spots[1]].set(high)


def levels(key, dims, cuts, low, top_value):
    level, own = 1.0, jax.random.fold_in(key, 6)
    for dim, blocks in cuts:
        steps = jnp.exp(jax.random.uniform(jax.random.fold_in(own, dim), (blocks,), jnp.float32, low / len(cuts), top_value / len(cuts)))
        level = level * jnp.repeat(steps, dims[dim] // blocks).reshape([-1 if axis == dim else 1 for axis in range(len(dims))])
    return level


def length_profile(number_of, total, bound, slope):
    portions = [(1 << 20) // math.isqrt(standing ** slope) + 1 for standing in range(2, number_of + 1)]
    rest, holding = total - bound - (number_of - 1), [1] * (number_of - 1)
    while rest > 0:
        candidates = [i for i in range(number_of - 1) if holding[i] < bound]
        pool, left = sum([portions[i] for i in candidates]), rest
        for i in candidates:
            extra = min(bound - holding[i], max(1, left * portions[i] // pool), rest)
            holding[i] = holding[i] + extra
            rest = rest - extra
    return np.array([bound] + holding)


def uneven(key, number_of, total, bound, slope):
    if number_of == 2:
        one = jax.random.randint(key, (), max(1, total - bound), min(bound, total - 1) + 1)
        return jnp.stack([one, total - one])
    tallies = jnp.asarray(length_profile(number_of, total, bound, slope), jnp.int32)
    couples = (number_of - 1) // 2
    giver, sink = tallies[1:1 + 2 * couples:2], tallies[2:2 + 2 * couples:2]
    margin = jnp.minimum(giver - 1, bound - sink)
    passed = jax.random.randint(jax.random.fold_in(key, 1), (couples,), 0, 1 << 20) % (margin + 1)
    tallies = tallies.at[1:1 + 2 * couples:2].set(giver - passed).at[2:2 + 2 * couples:2].set(sink + passed)
    return tallies[jax.random.permutation(jax.random.fold_in(key, 2), number_of)]


def bell_draw(key, dims, width, reach, pieces=(), kind=jnp.bfloat16):
    level = levels(key, dims, pieces, -0.22, 0.18) if pieces else 1.0
    values = jax.random.normal(key, dims, jnp.float32) * width * level
    return jnp.minimum(jnp.maximum(values, -reach), reach).astype(kind)


def setup_inputs(seed: int = 0) -> dict:
    splits = jax.random.split(jax.random.key(seed), 7)
    queries = draw_queries(jax.random.fold_in(splits[6], 71), 0)
    exponents = touch_ends(jax.random.randint(splits[1], (TOKENS, HEADS), -2, 3), jax.random.fold_in(splits[1], 1), -2, 2).astype(jnp.int32)
    latent = draw_latent(jax.random.fold_in(splits[6], 71), 0)
    segments = jnp.searchsorted(jnp.cumsum(uneven(splits[3], 3 * N_BLK, TOKENS, MOST, 0)), jnp.arange(TOKENS), side="right").astype(jnp.int32)
    key_weight = bell_draw(splits[4], (LATENT, HEADS * NOPE), LATENT ** -0.5, 0.25, ((1, 8),))
    value_weight = bell_draw(splits[5], (LATENT, HEADS * VDIM), LATENT ** -0.5, 0.25, ((1, 8),))
    return {"queries": queries, "exponents": exponents, "latent": latent, "segments": segments, "key_weight": key_weight, "value_weight": value_weight}


def power_two(exponent):
    result = jnp.zeros(exponent.shape, jnp.float32)
    for level in range(-4, 5):
        result = result + jnp.where(exponent == level, jnp.float32(2.0 ** level), jnp.float32(0.0))
    return result


def reference(queries, exponents, latent, segments, key_weight, value_weight):
    total = queries.shape[0]
    shaped = queries.reshape(total, HEADS, NOPE + ROPE).astype(jnp.float32)
    scaled = (shaped * power_two(exponents)[:, :, None]).astype(jnp.bfloat16)
    padded = jnp.concatenate([jnp.zeros((LEAD, LATENT + ROPE), jnp.bfloat16), latent], axis=0)
    compressed = padded[:, :LATENT]
    rope_keys = padded[:, LATENT:]
    padded_seg = jnp.concatenate([jnp.full((LEAD,), -1, jnp.int32), segments.astype(jnp.int32)], axis=0)
    padded_pos = jnp.arange(total + LEAD, dtype=jnp.int32) - LEAD
    softmax_scale = 1.0 / (NOPE + ROPE) ** 0.5
    key_heads = key_weight.reshape(LATENT, HEADS, NOPE).transpose(1, 0, 2)
    value_heads = value_weight.reshape(LATENT, HEADS, VDIM).transpose(1, 0, 2)
    query_heads = scaled.transpose(1, 0, 2)
    block_count = total // BLOCK

    def one_head(items):
        key_part, value_part, query_part = items
        keys = jnp.dot(compressed, key_part, preferred_element_type=jnp.float32).astype(jnp.bfloat16)
        values = jnp.dot(compressed, value_part, preferred_element_type=jnp.float32).astype(jnp.bfloat16)

        def one_block(index):
            start = (index * BLOCK).astype(jnp.int32)
            query_rows = lax.dynamic_slice_in_dim(query_part, start, BLOCK, 0)
            query_seg = lax.dynamic_slice_in_dim(padded_seg, start + LEAD, BLOCK, 0)
            query_pos = lax.dynamic_slice_in_dim(padded_pos, start + LEAD, BLOCK, 0)
            key_rows = lax.dynamic_slice_in_dim(keys, start, LEAD + BLOCK, 0)
            rope_rows = lax.dynamic_slice_in_dim(rope_keys, start, LEAD + BLOCK, 0)
            value_rows = lax.dynamic_slice_in_dim(values, start, LEAD + BLOCK, 0)
            key_seg = lax.dynamic_slice_in_dim(padded_seg, start, LEAD + BLOCK, 0)
            key_pos = lax.dynamic_slice_in_dim(padded_pos, start, LEAD + BLOCK, 0)
            allowed = (key_seg[None, :] == query_seg[:, None]) & (key_pos[None, :] <= query_pos[:, None]) & (key_pos[None, :] >= 0)
            scores = jnp.dot(query_rows[:, :NOPE], key_rows.T, preferred_element_type=jnp.float32)
            scores = scores + jnp.dot(query_rows[:, NOPE:], rope_rows.T, preferred_element_type=jnp.float32)
            scores = jnp.where(allowed, scores * softmax_scale, -1e30)
            largest = jnp.max(scores, axis=1, keepdims=True)
            weights = jnp.where(allowed, jnp.exp(scores - largest), 0.0)
            sums = jnp.sum(weights, axis=1, keepdims=True)
            weighted = jnp.dot(weights.astype(jnp.bfloat16), value_rows, preferred_element_type=jnp.float32)
            return (weighted / sums).astype(jnp.bfloat16)

        blocks = lax.map(one_block, jnp.arange(block_count, dtype=jnp.int32))
        return blocks.reshape(total, VDIM)

    outputs = lax.map(one_head, (key_heads, value_heads, query_heads))
    return outputs.transpose(1, 0, 2).reshape(total, HEADS * VDIM)
```

```python
import functools
import math

import jax
import jax.numpy as jnp
from jax import lax
from jax.experimental import pallas as pl
from jax.experimental.pallas import tpu as pltpu
from jax.sharding import PartitionSpec as P

NOPE = 128
ROPE = 64
LATENT = 512
VDIM = 128
LANES = 128
MINUS = -1e30


def power_two(exponent):
    result = jnp.zeros(exponent.shape, jnp.float32)
    for level in range(-4, 5):
        result = result + jnp.where(exponent == level, jnp.float32(2.0**level), jnp.float32(0.0))
    return result


def scale_kernel(distances, local, scal, queries, exponents, *outs):
    rows = queries.shape[0]
    heads = exponents.shape[1]
    width = local * (NOPE + ROPE)
    powers = power_two(exponents[...]).astype(jnp.bfloat16)
    lane = lax.broadcasted_iota(jnp.int32, (rows, LANES), 1)
    low = lane < ROPE
    from_head = lax.broadcasted_iota(jnp.int32, (heads, local * LANES), 0)
    to_head = lax.broadcasted_iota(jnp.int32, (heads, local * LANES), 1) // LANES
    for distance, out in zip(distances, outs):
        target = scal[0] ^ distance
        spread = jnp.where(from_head == to_head + target * local, 1.0, 0.0).astype(jnp.bfloat16)
        factor = jnp.dot(powers, spread, preferred_element_type=jnp.float32)
        first = pl.multiple_of(target * width, LANES)
        for pair in range(local // 2):
            base = pair * 3 * LANES
            one, two, three = (
                queries[:, pl.ds(first + base + k * LANES, LANES)].astype(jnp.float32) for k in range(3)
            )
            even = factor[:, 2 * pair * LANES : (2 * pair + 1) * LANES]
            odd = factor[:, (2 * pair + 1) * LANES : (2 * pair + 2) * LANES]
            nope_odd = pltpu.roll(jnp.where(low, three, two), ROPE, 1)
            ropes = jnp.where(low, two, three) * jnp.where(low, even, odd)
            at = 2 * pair * LANES
            out[:, at : at + LANES] = (one * even).astype(jnp.bfloat16)
            out[:, at + LANES : at + 2 * LANES] = (nope_odd * odd).astype(jnp.bfloat16)
            at = (local + pair) * LANES
            out[:, at : at + LANES] = ropes.astype(jnp.bfloat16)


def latent_kernel(latent, segments, out):
    rows = latent.shape[0]
    width = LATENT + ROPE
    square = lax.broadcasted_iota(jnp.int32, (rows, rows), 0) == lax.broadcasted_iota(jnp.int32, (rows, rows), 1)
    column = jnp.sum(jnp.where(square, segments[...].astype(jnp.float32), 0.0), axis=1, keepdims=True) + 1.0
    lane = lax.broadcasted_iota(jnp.int32, (rows, ROPE), 1)
    out[:, :width] = latent[...]
    out[:, width:] = jnp.where(lane == 0, column, 0.0).astype(jnp.bfloat16)


def project_kernel(rows, chips, scal, mine, theirs, key_weight, value_weight, keys, values, tail, window):
    place, core = scal[0] // 2, scal[0] % 2
    lead = chips * rows
    other_half = jnp.where(place < chips // 2, chips // 2, 0)
    for slot in range(chips + chips // 2):
        if slot < chips:
            to = lead + (place ^ slot) * 2 * rows
        else:
            to = ((place ^ (other_half + slot - chips)) - chips // 2) * 2 * rows
        take = slice(slot * rows, (slot + 1) * rows)
        window[pl.ds(pl.multiple_of(to + core * rows, rows), rows), :] = mine[take, :]
        window[pl.ds(pl.multiple_of(to + (1 - core) * rows, rows), rows), :] = theirs[take, :]
    tail[...] = window[:, LATENT:]
    columns = keys.shape[1]
    tile = min(256, columns)
    step_rows = 256

    def one(step, carry):
        at = pl.multiple_of(step * tile, tile)
        for start in range(0, window.shape[0], step_rows):
            part = window[start : start + step_rows, :LATENT]
            for weight, out in ((key_weight, keys), (value_weight, values)):
                out[start : start + step_rows, pl.ds(at, tile)] = jnp.dot(
                    part, weight[:, pl.ds(at, tile)], preferred_element_type=jnp.float32
                ).astype(jnp.bfloat16)
        return carry

    lax.fori_loop(0, columns // tile, one, 0)


def attend_kernel(rows, chips, local, slot, scal, mine, theirs, keys, values, tail, out_mine, out_theirs):
    place, core = scal[0] // 2, scal[0] % 2
    lead = chips * rows
    chip = place ^ slot
    block = 2 * rows
    width = lead + block
    start = pl.multiple_of(chip * block, block)
    own = pl.multiple_of(lead + start + core * rows, rows)
    other = pl.multiple_of(lead + start + (1 - core) * rows, rows)
    key_tail = tail[pl.ds(start, width), :]
    pick = jnp.where(lax.broadcasted_iota(jnp.int32, (8, LANES), 1) == ROPE, 1.0, 0.0).astype(jnp.bfloat16)
    key_seg = lax.dot_general(pick, key_tail, (((1,), (1,)), ((), ())), preferred_element_type=jnp.float32)[0:1]
    query_tail = jnp.concatenate([tail[pl.ds(own, rows), :], tail[pl.ds(other, rows), :]], axis=0)
    query_seg = query_tail[:, ROPE : ROPE + 1].astype(jnp.float32)
    row = lax.broadcasted_iota(jnp.int32, (block, width), 0)
    column = lax.broadcasted_iota(jnp.int32, (block, width), 1)
    shift = jnp.where(row < rows, core * rows, -core * rows)
    bias = jnp.where((query_seg == key_seg) & (column <= row + shift + lead), 0.0, MINUS)
    lane = lax.broadcasted_iota(jnp.int32, (width, LANES), 1)
    rope_even = jnp.where(lane < ROPE, key_tail.astype(jnp.float32), 0.0)
    rope_odd = pltpu.roll(rope_even, ROPE, 1)
    rope = (rope_even.astype(jnp.bfloat16), rope_odd.astype(jnp.bfloat16))
    factor = math.log2(math.e) / math.sqrt(NOPE + ROPE)
    for head in range(local):
        at = slice(head * LANES, (head + 1) * LANES)
        pair = slice((local + head // 2) * LANES, (local + head // 2 + 1) * LANES)
        query = jnp.concatenate(
            [
                jnp.concatenate([mine[:, at], mine[:, pair]], axis=1),
                jnp.concatenate([theirs[:, at], theirs[:, pair]], axis=1),
            ],
            axis=0,
        )
        key = jnp.concatenate([keys[pl.ds(start, width), at], rope[head % 2]], axis=1)
        scores = lax.dot_general(query, key, (((1,), (1,)), ((), ())), preferred_element_type=jnp.float32)
        scores = scores * factor + bias
        largest = jnp.max(scores, axis=1, keepdims=True)
        weights = jnp.exp2(scores - largest)
        inverse = 1.0 / jnp.sum(weights, axis=1, keepdims=True)
        weighted = jnp.dot(
            weights.astype(jnp.bfloat16), values[pl.ds(start, width), at], preferred_element_type=jnp.float32
        )
        result = (weighted * inverse).astype(jnp.bfloat16)
        out_mine[:, at] = result[:rows]
        out_theirs[:, at] = result[rows:]


def join_kernel(scal, *refs):
    pieces, out = refs[:-1], refs[-1]
    width = pieces[0].shape[1]
    for distance, piece in enumerate(pieces):
        out[:, pl.ds(pl.multiple_of((scal[0] ^ distance) * width, LANES), width)] = piece[...]


def call(kernel, outs, *args, scratch=(), flops=0, nbytes=0, exps=0, scalar=True):
    vmem = pl.BlockSpec(memory_space=pltpu.VMEM)
    smem = pl.BlockSpec(memory_space=pltpu.SMEM)
    specs = [smem if scalar and k == 0 else vmem for k in range(len(args))]
    shapes = [jax.ShapeDtypeStruct(shape, jnp.bfloat16) for shape in outs]
    return pl.pallas_call(
        kernel,
        out_shape=shapes,
        in_specs=specs,
        out_specs=[vmem] * len(outs),
        scratch_shapes=list(scratch),
        cost_estimate=pl.CostEstimate(flops=flops, bytes_accessed=nbytes, transcendentals=exps),
    )(*args)


def body(queries, exponents, latent, segments, key_weight, value_weight):
    rows = queries.shape[0]
    heads = exponents.shape[1]
    count = lax.axis_size("head")
    blocks = lax.axis_size("blk")
    local = heads // count
    width = queries.shape[1] // count
    chips = count // 2
    lead = chips * rows
    window_rows = 3 * lead
    columns = local * VDIM
    position = lax.axis_index("head").astype(jnp.int32)
    scal = position.reshape(1)

    def swap(block, distance):
        return lax.ppermute(block, "head", [(i, i ^ distance) for i in range(count)])

    (padded,) = call(
        latent_kernel, [(rows, LATENT + 2 * ROPE)], latent, segments.reshape(1, rows), scalar=False, nbytes=200000
    )
    far = list(range(chips, count))
    near = list(range(chips))
    piece = (rows, width)
    far_pieces = call(
        functools.partial(scale_kernel, far, local), [piece] * len(far), scal, queries, exponents, nbytes=2000000
    )
    near_pieces = call(
        functools.partial(scale_kernel, near, local), [piece] * len(near), scal, queries, exponents, nbytes=2000000
    )
    sent = near_pieces + far_pieces

    own = [padded] + [swap(padded, 2 * k) for k in range(1, chips)]
    own = jnp.concatenate(own, axis=0)
    other_half = jnp.where(position // 2 < chips // 2, chips // 2, 0)
    upper = lax.dynamic_slice_in_dim(own, other_half * rows, chips // 2 * rows, 0)
    earlier = lax.ppermute(upper, "blk", [(i, i + 1) for i in range(blocks - 1)])
    mine = jnp.concatenate([own, earlier], axis=0)
    theirs = swap(mine, 1)

    arrived = [None] * count
    for distance in far + near[2:] + near[:2]:
        arrived[distance] = sent[distance] if distance == 0 else swap(sent[distance], distance)

    keys, values, tail = call(
        functools.partial(project_kernel, rows, chips),
        [(window_rows, columns), (window_rows, columns), (window_rows, LANES)],
        scal,
        mine,
        theirs,
        key_weight,
        value_weight,
        scratch=[pltpu.VMEM((window_rows, LATENT + LANES), jnp.bfloat16)],
        flops=4 * window_rows * LATENT * columns,
        nbytes=4 * LATENT * columns,
    )

    returned = [None] * count
    span = lead + 2 * rows
    for slot in list(range(chips // 2, chips)) + list(range(1, chips // 2)) + [0]:
        results = call(
            functools.partial(attend_kernel, rows, chips, local, slot),
            [(rows, columns)] * 2,
            scal,
            arrived[2 * slot],
            arrived[2 * slot + 1],
            keys,
            values,
            tail,
            flops=2 * 2 * rows * span * local * 384,
            nbytes=4 * rows * (width + columns),
            exps=2 * rows * span * local,
        )
        for distance, result in zip((2 * slot, 2 * slot + 1), results):
            returned[distance] = result if distance == 0 else swap(result, distance)
    (joined,) = call(join_kernel, [(rows, heads * VDIM)], scal, *returned, nbytes=4 * rows * heads * VDIM)
    return joined


def solution(mesh):
    in_specs = (
        P(("blk", "head"), None),
        P(("blk", "head"), None),
        P(("blk", "head"), None),
        P(("blk", "head")),
        P(None, "head"),
        P(None, "head"),
    )
    out_specs = P(("blk", "head"), None)
    return jax.shard_map(body, mesh=mesh, in_specs=in_specs, out_specs=out_specs, check_vma=False)
```

```python
import functools
import math

import jax
import jax.numpy as jnp
from jax import lax
from jax.experimental import pallas as pl
from jax.experimental.pallas import tpu as pltpu
from jax.sharding import PartitionSpec as P


NOPE = 128
ROPE = 64
LATENT = 512
VDIM = 128
LANES = 128
MINUS = -1e30
GRANT = 16 * 1024 * 1024


def power_two(exponent):
    result = jnp.zeros(exponent.shape, jnp.float32)
    for level in range(-4, 5):
        result = result + jnp.where(exponent == level, jnp.float32(2.0**level), jnp.float32(0.0))
    return result


def scale_part(distances, local, scal, queries, exponents, outs):
    rows = queries.shape[0]
    heads = exponents.shape[1]
    width = local * (NOPE + ROPE)
    powers = power_two(exponents[...]).astype(jnp.bfloat16)
    lane = lax.broadcasted_iota(jnp.int32, (rows, LANES), 1)
    low = lane < ROPE
    from_head = lax.broadcasted_iota(jnp.int32, (heads, local * LANES), 0)
    to_head = lax.broadcasted_iota(jnp.int32, (heads, local * LANES), 1) // LANES
    for distance, out in zip(distances, outs):
        target = scal[0] ^ distance
        spread = jnp.where(from_head == to_head + target * local, 1.0, 0.0).astype(jnp.bfloat16)
        factor = jnp.dot(powers, spread, preferred_element_type=jnp.float32)
        first = pl.multiple_of(target * width, LANES)
        for pair in range(local // 2):
            base = pair * 3 * LANES
            one, two, three = (
                queries[:, pl.ds(first + base + k * LANES, LANES)].astype(jnp.float32) for k in range(3)
            )
            even = factor[:, 2 * pair * LANES : (2 * pair + 1) * LANES]
            odd = factor[:, (2 * pair + 1) * LANES : (2 * pair + 2) * LANES]
            nope_odd = pltpu.roll(jnp.where(low, three, two), ROPE, 1)
            ropes = jnp.where(low, two, three) * jnp.where(low, even, odd)
            at = 2 * pair * LANES
            out[:, at : at + LANES] = (one * even).astype(jnp.bfloat16)
            out[:, at + LANES : at + 2 * LANES] = (nope_odd * odd).astype(jnp.bfloat16)
            at = (local + pair) * LANES
            out[:, at : at + LANES] = ropes.astype(jnp.bfloat16)


def latent_part(latent, segments, out):
    rows = latent.shape[0]
    width = LATENT + ROPE
    square = lax.broadcasted_iota(jnp.int32, (rows, rows), 0) == lax.broadcasted_iota(jnp.int32, (rows, rows), 1)
    column = jnp.sum(jnp.where(square, segments[...].astype(jnp.float32), 0.0), axis=1, keepdims=True) + 1.0
    lane = lax.broadcasted_iota(jnp.int32, (rows, ROPE), 1)
    out[:, :width] = latent[...]
    out[:, width:] = jnp.where(lane == 0, column, 0.0).astype(jnp.bfloat16)


def prepare_kernel(distances, local, scal, queries, exponents, latent, segments, padded, *outs):
    latent_part(latent, segments, padded)
    scale_part(distances, local, scal, queries, exponents, outs)


def scale_kernel(distances, local, scal, queries, exponents, *outs):
    scale_part(distances, local, scal, queries, exponents, outs)


def project_kernel(rows, chips, scal, mine, theirs, key_weight, value_weight, keys, values, tail, window):
    place, core = scal[0] // 2, scal[0] % 2
    lead = chips * rows
    other_half = jnp.where(place < chips // 2, chips // 2, 0)
    for slot in range(chips + chips // 2):
        if slot < chips:
            to = lead + (place ^ slot) * 2 * rows
        else:
            to = ((place ^ (other_half + slot - chips)) - chips // 2) * 2 * rows
        take = slice(slot * rows, (slot + 1) * rows)
        window[pl.ds(pl.multiple_of(to + core * rows, rows), rows), :] = mine[take, :]
        window[pl.ds(pl.multiple_of(to + (1 - core) * rows, rows), rows), :] = theirs[take, :]
    tail[...] = window[:, LATENT:]
    columns = keys.shape[1]
    tile = min(256, columns)
    step_rows = 256

    def one(step, carry):
        at = pl.multiple_of(step * tile, tile)
        for start in range(0, window.shape[0], step_rows):
            part = window[start : start + step_rows, :LATENT]
            for weight, out in ((key_weight, keys), (value_weight, values)):
                out[start : start + step_rows, pl.ds(at, tile)] = jnp.dot(
                    part, weight[:, pl.ds(at, tile)], preferred_element_type=jnp.float32
                ).astype(jnp.bfloat16)
        return carry

    lax.fori_loop(0, columns // tile, one, 0)


def attend_kernel(rows, chips, local, slot, scal, mine, theirs, keys, values, tail, out_mine, out_theirs):
    place, core = scal[0] // 2, scal[0] % 2
    lead = chips * rows
    chip = place ^ slot
    block = 2 * rows
    width = lead + block
    start = pl.multiple_of(chip * block, block)
    own = pl.multiple_of(lead + start + core * rows, rows)
    other = pl.multiple_of(lead + start + (1 - core) * rows, rows)
    key_tail = tail[pl.ds(start, width), :]
    pick = jnp.where(lax.broadcasted_iota(jnp.int32, (8, LANES), 1) == ROPE, 1.0, 0.0).astype(jnp.bfloat16)
    key_seg = lax.dot_general(pick, key_tail, (((1,), (1,)), ((), ())), preferred_element_type=jnp.float32)[0:1]
    query_tail = jnp.concatenate([tail[pl.ds(own, rows), :], tail[pl.ds(other, rows), :]], axis=0)
    query_seg = query_tail[:, ROPE : ROPE + 1].astype(jnp.float32)
    row = lax.broadcasted_iota(jnp.int32, (block, width), 0)
    column = lax.broadcasted_iota(jnp.int32, (block, width), 1)
    shift = jnp.where(row < rows, core * rows, -core * rows)
    bias = jnp.where((query_seg == key_seg) & (column <= row + shift + lead), 0.0, MINUS)
    lane = lax.broadcasted_iota(jnp.int32, (width, LANES), 1)
    rope_even = jnp.where(lane < ROPE, key_tail.astype(jnp.float32), 0.0)
    rope_odd = pltpu.roll(rope_even, ROPE, 1)
    rope = (rope_even.astype(jnp.bfloat16), rope_odd.astype(jnp.bfloat16))
    factor = math.log2(math.e) / math.sqrt(NOPE + ROPE)
    for head in range(local):
        at = slice(head * LANES, (head + 1) * LANES)
        pair = slice((local + head // 2) * LANES, (local + head // 2 + 1) * LANES)
        query = jnp.concatenate(
            [
                jnp.concatenate([mine[:, at], mine[:, pair]], axis=1),
                jnp.concatenate([theirs[:, at], theirs[:, pair]], axis=1),
            ],
            axis=0,
        )
        key = jnp.concatenate([keys[pl.ds(start, width), at], rope[head % 2]], axis=1)
        scores = lax.dot_general(query, key, (((1,), (1,)), ((), ())), preferred_element_type=jnp.float32)
        scores = scores * factor + bias
        largest = jnp.max(scores, axis=1, keepdims=True)
        weights = jnp.exp2(scores - largest)
        inverse = 1.0 / jnp.sum(weights, axis=1, keepdims=True)
        weighted = jnp.dot(
            weights.astype(jnp.bfloat16), values[pl.ds(start, width), at], preferred_element_type=jnp.float32
        )
        result = (weighted * inverse).astype(jnp.bfloat16)
        out_mine[:, at] = result[:rows]
        out_theirs[:, at] = result[rows:]


def join_kernel(scal, *refs):
    pieces, out = refs[:-1], refs[-1]
    width = pieces[0].shape[1]
    for distance, piece in enumerate(pieces):
        out[:, pl.ds(pl.multiple_of((scal[0] ^ distance) * width, LANES), width)] = piece[...]


def call(kernel, outs, *args, scratch=(), flops=0, nbytes=0, exps=0):
    vmem = pl.BlockSpec(memory_space=pltpu.VMEM)
    smem = pl.BlockSpec(memory_space=pltpu.SMEM)
    specs = [smem] + [vmem] * (len(args) - 1)
    shapes = [jax.ShapeDtypeStruct(shape, jnp.bfloat16) for shape in outs]
    return pl.pallas_call(
        kernel,
        out_shape=shapes,
        in_specs=specs,
        out_specs=[vmem] * len(outs),
        scratch_shapes=list(scratch),
        cost_estimate=pl.CostEstimate(flops=flops, bytes_accessed=nbytes, transcendentals=exps),
        compiler_params=pltpu.CompilerParams(vmem_limit_bytes=GRANT),
    )(*args)


def layer(queries, exponents, latent, segments, key_weight, value_weight):
    rows = queries.shape[0]
    heads = exponents.shape[1]
    count = lax.axis_size("head")
    blocks = lax.axis_size("blk")
    local = heads // count
    width = queries.shape[1] // count
    chips = count // 2
    lead = chips * rows
    window_rows = 3 * lead
    columns = local * VDIM
    position = lax.axis_index("head").astype(jnp.int32)
    scal = position.reshape(1)

    def swap(block, distance):
        return lax.ppermute(block, "head", [(i, i ^ distance) for i in range(count)])

    far = list(range(chips, count))
    near = list(range(chips))
    piece = (rows, width)
    padded, *far_pieces = call(
        functools.partial(prepare_kernel, far, local),
        [(rows, LATENT + 2 * ROPE)] + [piece] * len(far),
        scal,
        queries,
        exponents,
        latent,
        segments.reshape(1, rows),
        nbytes=2000000,
    )
    near_pieces = call(
        functools.partial(scale_kernel, near, local), [piece] * len(near), scal, queries, exponents, nbytes=2000000
    )
    sent = list(near_pieces) + list(far_pieces)

    own = [padded] + [swap(padded, 2 * k) for k in range(1, chips)]
    own = jnp.concatenate(own, axis=0)
    other_half = jnp.where(position // 2 < chips // 2, chips // 2, 0)
    upper = lax.dynamic_slice_in_dim(own, other_half * rows, chips // 2 * rows, 0)
    earlier = lax.ppermute(upper, "blk", [(i, i + 1) for i in range(blocks - 1)])
    mine = jnp.concatenate([own, earlier], axis=0)
    theirs = swap(mine, 1)

    arrived = [sent[0]] + [swap(sent[distance], distance) for distance in range(1, count)]

    keys, values, tail = call(
        functools.partial(project_kernel, rows, chips),
        [(window_rows, columns), (window_rows, columns), (window_rows, LANES)],
        scal,
        mine,
        theirs,
        key_weight,
        value_weight,
        scratch=[pltpu.VMEM((window_rows, LATENT + LANES), jnp.bfloat16)],
        flops=4 * window_rows * LATENT * columns,
        nbytes=4 * LATENT * columns,
    )

    returned = [None] * count
    span = lead + 2 * rows
    for slot in range(chips):
        results = call(
            functools.partial(attend_kernel, rows, chips, local, slot),
            [(rows, columns)] * 2,
            scal,
            arrived[2 * slot],
            arrived[2 * slot + 1],
            keys,
            values,
            tail,
            flops=2 * 2 * rows * span * local * 384,
            nbytes=4 * rows * (width + columns),
            exps=2 * rows * span * local,
        )
        for distance, result in zip((2 * slot, 2 * slot + 1), results):
            returned[distance] = result if distance == 0 else swap(result, distance)
    (joined,) = call(join_kernel, [(rows, heads * VDIM)], scal, *returned, nbytes=4 * rows * heads * VDIM)
    return joined


def solution(mesh):
    in_specs = (
        P(("blk", "head"), None),
        P(("blk", "head"), None),
        P(("blk", "head"), None),
        P(("blk", "head")),
        P(None, "head"),
        P(None, "head"),
    )
    out_specs = P(("blk", "head"), None)
    return jax.shard_map(layer, mesh=mesh, in_specs=in_specs, out_specs=out_specs, check_vma=False)
```

```python
import functools
import math

import jax
import jax.numpy as jnp
from jax import lax
from jax.experimental import pallas as pl
from jax.experimental.pallas import tpu as pltpu
from jax.sharding import PartitionSpec as P


NOPE = 128
ROPE = 64
LATENT = 512
VDIM = 128
LANES = 128
MINUS = -1e30
GRANT = 16 * 1024 * 1024


def power_two(exponent):
    result = jnp.zeros(exponent.shape, jnp.float32)
    for level in range(-4, 5):
        result = result + jnp.where(exponent == level, jnp.float32(2.0**level), jnp.float32(0.0))
    return result


def scale_part(distances, local, scal, queries, exponents, outs):
    rows = queries.shape[0]
    heads = exponents.shape[1]
    width = local * (NOPE + ROPE)
    powers = power_two(exponents[...]).astype(jnp.bfloat16)
    lane = lax.broadcasted_iota(jnp.int32, (rows, LANES), 1)
    low = lane < ROPE
    from_head = lax.broadcasted_iota(jnp.int32, (heads, local * LANES), 0)
    to_head = lax.broadcasted_iota(jnp.int32, (heads, local * LANES), 1) // LANES
    for distance, out in zip(distances, outs):
        target = scal[0] ^ distance
        spread = jnp.where(from_head == to_head + target * local, 1.0, 0.0).astype(jnp.bfloat16)
        factor = jnp.dot(powers, spread, preferred_element_type=jnp.float32)
        first = pl.multiple_of(target * width, LANES)
        for pair in range(local // 2):
            base = pair * 3 * LANES
            one, two, three = (
                queries[:, pl.ds(first + base + k * LANES, LANES)].astype(jnp.float32) for k in range(3)
            )
            even = factor[:, 2 * pair * LANES : (2 * pair + 1) * LANES]
            odd = factor[:, (2 * pair + 1) * LANES : (2 * pair + 2) * LANES]
            nope_odd = pltpu.roll(jnp.where(low, three, two), ROPE, 1)
            ropes = jnp.where(low, two, three) * jnp.where(low, even, odd)
            at = 2 * pair * LANES
            out[:, at : at + LANES] = (one * even).astype(jnp.bfloat16)
            out[:, at + LANES : at + 2 * LANES] = (nope_odd * odd).astype(jnp.bfloat16)
            at = (local + pair) * LANES
            out[:, at : at + LANES] = ropes.astype(jnp.bfloat16)


def latent_part(latent, segments, out):
    rows = latent.shape[0]
    width = LATENT + ROPE
    square = lax.broadcasted_iota(jnp.int32, (rows, rows), 0) == lax.broadcasted_iota(jnp.int32, (rows, rows), 1)
    column = jnp.sum(jnp.where(square, segments[...].astype(jnp.float32), 0.0), axis=1, keepdims=True) + 1.0
    lane = lax.broadcasted_iota(jnp.int32, (rows, ROPE), 1)
    out[:, :width] = latent[...]
    out[:, width:] = jnp.where(lane == 0, column, 0.0).astype(jnp.bfloat16)


def prepare_kernel(distances, local, scal, queries, exponents, latent, segments, padded, *rest):
    outs, (queries_here, exponents_here, latent_here, segments_here, sems) = rest[:-5], rest[-5:]
    copies = [
        pltpu.make_async_copy(source, target, sems.at[k])
        for k, (source, target) in enumerate(
            (
                (latent, latent_here),
                (segments, segments_here),
                (exponents, exponents_here),
                (queries, queries_here),
            )
        )
    ]
    for copy in copies:
        copy.start()
    copies[0].wait()
    copies[1].wait()
    latent_part(latent_here, segments_here, padded)
    copies[2].wait()
    copies[3].wait()
    scale_part(distances, local, scal, queries_here, exponents_here, outs)


def scale_kernel(distances, local, scal, queries, exponents, *rest):
    outs, (queries_here, exponents_here, sems) = rest[:-3], rest[-3:]
    copies = [
        pltpu.make_async_copy(exponents, exponents_here, sems.at[0]),
        pltpu.make_async_copy(queries, queries_here, sems.at[1]),
    ]
    for copy in copies:
        copy.start()
    for copy in copies:
        copy.wait()
    scale_part(distances, local, scal, queries_here, exponents_here, outs)


def project_kernel(rows, chips, scal, mine, theirs, key_weight, value_weight, keys, values, tail, window):
    place, core = scal[0] // 2, scal[0] % 2
    lead = chips * rows
    other_half = jnp.where(place < chips // 2, chips // 2, 0)
    for slot in range(chips + chips // 2):
        if slot < chips:
            to = lead + (place ^ slot) * 2 * rows
        else:
            to = ((place ^ (other_half + slot - chips)) - chips // 2) * 2 * rows
        take = slice(slot * rows, (slot + 1) * rows)
        window[pl.ds(pl.multiple_of(to + core * rows, rows), rows), :] = mine[take, :]
        window[pl.ds(pl.multiple_of(to + (1 - core) * rows, rows), rows), :] = theirs[take, :]
    tail[...] = window[:, LATENT:]
    columns = keys.shape[1]
    tile = min(256, columns)
    step_rows = 256

    def one(step, carry):
        at = pl.multiple_of(step * tile, tile)
        for start in range(0, window.shape[0], step_rows):
            part = window[start : start + step_rows, :LATENT]
            for weight, out in ((key_weight, keys), (value_weight, values)):
                out[start : start + step_rows, pl.ds(at, tile)] = jnp.dot(
                    part, weight[:, pl.ds(at, tile)], preferred_element_type=jnp.float32
                ).astype(jnp.bfloat16)
        return carry

    lax.fori_loop(0, columns // tile, one, 0)


def attend_kernel(rows, chips, local, slot, scal, mine, theirs, keys, values, tail, out_mine, out_theirs):
    place, core = scal[0] // 2, scal[0] % 2
    lead = chips * rows
    chip = place ^ slot
    block = 2 * rows
    width = lead + block
    start = pl.multiple_of(chip * block, block)
    own = pl.multiple_of(lead + start + core * rows, rows)
    other = pl.multiple_of(lead + start + (1 - core) * rows, rows)
    key_tail = tail[pl.ds(start, width), :]
    pick = jnp.where(lax.broadcasted_iota(jnp.int32, (8, LANES), 1) == ROPE, 1.0, 0.0).astype(jnp.bfloat16)
    key_seg = lax.dot_general(pick, key_tail, (((1,), (1,)), ((), ())), preferred_element_type=jnp.float32)[0:1]
    query_tail = jnp.concatenate([tail[pl.ds(own, rows), :], tail[pl.ds(other, rows), :]], axis=0)
    query_seg = query_tail[:, ROPE : ROPE + 1].astype(jnp.float32)
    row = lax.broadcasted_iota(jnp.int32, (block, width), 0)
    column = lax.broadcasted_iota(jnp.int32, (block, width), 1)
    shift = jnp.where(row < rows, core * rows, -core * rows)
    bias = jnp.where((query_seg == key_seg) & (column <= row + shift + lead), 0.0, MINUS)
    lane = lax.broadcasted_iota(jnp.int32, (width, LANES), 1)
    rope_even = jnp.where(lane < ROPE, key_tail.astype(jnp.float32), 0.0)
    rope_odd = pltpu.roll(rope_even, ROPE, 1)
    rope = (rope_even.astype(jnp.bfloat16), rope_odd.astype(jnp.bfloat16))
    factor = math.log2(math.e) / math.sqrt(NOPE + ROPE)
    for head in range(local):
        at = slice(head * LANES, (head + 1) * LANES)
        pair = slice((local + head // 2) * LANES, (local + head // 2 + 1) * LANES)
        query = jnp.concatenate(
            [
                jnp.concatenate([mine[:, at], mine[:, pair]], axis=1),
                jnp.concatenate([theirs[:, at], theirs[:, pair]], axis=1),
            ],
            axis=0,
        )
        key = jnp.concatenate([keys[pl.ds(start, width), at], rope[head % 2]], axis=1)
        scores = lax.dot_general(query, key, (((1,), (1,)), ((), ())), preferred_element_type=jnp.float32)
        scores = scores * factor + bias
        largest = jnp.max(scores, axis=1, keepdims=True)
        weights = jnp.exp2(scores - largest)
        inverse = 1.0 / jnp.sum(weights, axis=1, keepdims=True)
        weighted = jnp.dot(
            weights.astype(jnp.bfloat16), values[pl.ds(start, width), at], preferred_element_type=jnp.float32
        )
        result = (weighted * inverse).astype(jnp.bfloat16)
        out_mine[:, at] = result[:rows]
        out_theirs[:, at] = result[rows:]


def join_kernel(scal, *refs):
    pieces, out = refs[:-1], refs[-1]
    width = pieces[0].shape[1]
    for distance, piece in enumerate(pieces):
        out[:, pl.ds(pl.multiple_of((scal[0] ^ distance) * width, LANES), width)] = piece[...]


def call(kernel, outs, *args, scratch=(), flops=0, nbytes=0, exps=0, fetched=False):
    vmem = pl.BlockSpec(memory_space=pltpu.VMEM)
    smem = pl.BlockSpec(memory_space=pltpu.SMEM)
    hbm = pl.BlockSpec(memory_space=pltpu.HBM)
    specs = [smem] + [hbm if fetched else vmem] * (len(args) - 1)
    if fetched:
        scratch = [pltpu.VMEM(arg.shape, arg.dtype) for arg in args[1:]]
        scratch.append(pltpu.SemaphoreType.DMA((len(args) - 1,)))
        args = args[:1] + tuple(pltpu.with_memory_space_constraint(arg, pltpu.HBM) for arg in args[1:])
    shapes = [jax.ShapeDtypeStruct(shape, jnp.bfloat16) for shape in outs]
    return pl.pallas_call(
        kernel,
        out_shape=shapes,
        in_specs=specs,
        out_specs=[vmem] * len(outs),
        scratch_shapes=list(scratch),
        cost_estimate=pl.CostEstimate(flops=flops, bytes_accessed=nbytes, transcendentals=exps),
        compiler_params=pltpu.CompilerParams(vmem_limit_bytes=GRANT),
    )(*args)


def layer(queries, exponents, latent, segments, key_weight, value_weight):
    rows = queries.shape[0]
    heads = exponents.shape[1]
    count = lax.axis_size("head")
    blocks = lax.axis_size("blk")
    local = heads // count
    width = queries.shape[1] // count
    chips = count // 2
    lead = chips * rows
    window_rows = 3 * lead
    columns = local * VDIM
    position = lax.axis_index("head").astype(jnp.int32)
    scal = position.reshape(1)

    def swap(block, distance):
        return lax.ppermute(block, "head", [(i, i ^ distance) for i in range(count)])

    far = list(range(chips, count))
    near = list(range(chips))
    piece = (rows, width)
    padded, *far_pieces = call(
        functools.partial(prepare_kernel, far, local),
        [(rows, LATENT + 2 * ROPE)] + [piece] * len(far),
        scal,
        queries,
        exponents,
        latent,
        segments.reshape(1, rows),
        nbytes=2000000,
        fetched=True,
    )
    near_pieces = call(
        functools.partial(scale_kernel, near, local),
        [piece] * len(near),
        scal,
        queries,
        exponents,
        nbytes=2000000,
        fetched=True,
    )
    sent = list(near_pieces) + list(far_pieces)

    own = [padded] + [swap(padded, 2 * k) for k in range(1, chips)]
    own = jnp.concatenate(own, axis=0)
    other_half = jnp.where(position // 2 < chips // 2, chips // 2, 0)
    upper = lax.dynamic_slice_in_dim(own, other_half * rows, chips // 2 * rows, 0)
    earlier = lax.ppermute(upper, "blk", [(i, i + 1) for i in range(blocks - 1)])
    mine = jnp.concatenate([own, earlier], axis=0)
    theirs = swap(mine, 1)

    arrived = [sent[0]] + [swap(sent[distance], distance) for distance in range(1, count)]

    keys, values, tail = call(
        functools.partial(project_kernel, rows, chips),
        [(window_rows, columns), (window_rows, columns), (window_rows, LANES)],
        scal,
        mine,
        theirs,
        key_weight,
        value_weight,
        scratch=[pltpu.VMEM((window_rows, LATENT + LANES), jnp.bfloat16)],
        flops=4 * window_rows * LATENT * columns,
        nbytes=4 * LATENT * columns,
    )

    returned = [None] * count
    span = lead + 2 * rows
    for slot in range(chips):
        results = call(
            functools.partial(attend_kernel, rows, chips, local, slot),
            [(rows, columns)] * 2,
            scal,
            arrived[2 * slot],
            arrived[2 * slot + 1],
            keys,
            values,
            tail,
            flops=2 * 2 * rows * span * local * 384,
            nbytes=4 * rows * (width + columns),
            exps=2 * rows * span * local,
        )
        for distance, result in zip((2 * slot, 2 * slot + 1), results):
            returned[distance] = result if distance == 0 else swap(result, distance)
    (joined,) = call(join_kernel, [(rows, heads * VDIM)], scal, *returned, nbytes=4 * rows * heads * VDIM)
    return joined


def solution(mesh):
    in_specs = (
        P(("blk", "head"), None),
        P(("blk", "head"), None),
        P(("blk", "head"), None),
        P(("blk", "head")),
        P(None, "head"),
        P(None, "head"),
    )
    out_specs = P(("blk", "head"), None)
    return jax.shard_map(layer, mesh=mesh, in_specs=in_specs, out_specs=out_specs, check_vma=False)
```

```python
import functools
import math

import jax
import jax.numpy as jnp
from jax import lax
from jax.experimental import pallas as pl
from jax.experimental.pallas import tpu as pltpu
from jax.sharding import PartitionSpec as P


NOPE = 128
ROPE = 64
LATENT = 512
VDIM = 128
LANES = 128
MINUS = -1e30
GRANT = 16 * 1024 * 1024


def power_two(exponent):
    result = jnp.zeros(exponent.shape, jnp.float32)
    for level in range(-4, 5):
        result = result + jnp.where(exponent == level, jnp.float32(2.0**level), jnp.float32(0.0))
    return result


def scale_part(distances, local, scal, queries, exponents, outs):
    rows = queries.shape[0]
    heads = exponents.shape[1]
    width = local * (NOPE + ROPE)
    powers = power_two(exponents[...]).astype(jnp.bfloat16)
    lane = lax.broadcasted_iota(jnp.int32, (rows, LANES), 1)
    low = lane < ROPE
    from_head = lax.broadcasted_iota(jnp.int32, (heads, local * LANES), 0)
    to_head = lax.broadcasted_iota(jnp.int32, (heads, local * LANES), 1) // LANES
    for distance, out in zip(distances, outs):
        target = scal[0] ^ distance
        spread = jnp.where(from_head == to_head + target * local, 1.0, 0.0).astype(jnp.bfloat16)
        factor = jnp.dot(powers, spread, preferred_element_type=jnp.float32)
        first = pl.multiple_of(target * width, LANES)
        for pair in range(local // 2):
            base = pair * 3 * LANES
            one, two, three = (
                queries[:, pl.ds(first + base + k * LANES, LANES)].astype(jnp.float32) for k in range(3)
            )
            even = factor[:, 2 * pair * LANES : (2 * pair + 1) * LANES]
            odd = factor[:, (2 * pair + 1) * LANES : (2 * pair + 2) * LANES]
            nope_odd = pltpu.roll(jnp.where(low, three, two), ROPE, 1)
            ropes = jnp.where(low, two, three) * jnp.where(low, even, odd)
            at = 2 * pair * LANES
            out[:, at : at + LANES] = (one * even).astype(jnp.bfloat16)
            out[:, at + LANES : at + 2 * LANES] = (nope_odd * odd).astype(jnp.bfloat16)
            at = (local + pair) * LANES
            out[:, at : at + LANES] = ropes.astype(jnp.bfloat16)


def latent_part(latent, segments, out):
    rows = latent.shape[0]
    width = LATENT + ROPE
    square = lax.broadcasted_iota(jnp.int32, (rows, rows), 0) == lax.broadcasted_iota(jnp.int32, (rows, rows), 1)
    column = jnp.sum(jnp.where(square, segments[...].astype(jnp.float32), 0.0), axis=1, keepdims=True) + 1.0
    lane = lax.broadcasted_iota(jnp.int32, (rows, ROPE), 1)
    out[:, :width] = latent[...]
    out[:, width:] = jnp.where(lane == 0, column, 0.0).astype(jnp.bfloat16)


def prepare_kernel(distances, local, scal, queries, exponents, latent, segments, padded, *rest):
    outs, (queries_here, exponents_here, latent_here, segments_here, sems) = rest[:-5], rest[-5:]
    copies = [
        pltpu.make_async_copy(source, target, sems.at[k])
        for k, (source, target) in enumerate(
            (
                (latent, latent_here),
                (segments, segments_here),
                (exponents, exponents_here),
                (queries, queries_here),
            )
        )
    ]
    for copy in copies:
        copy.start()
    copies[0].wait()
    copies[1].wait()
    latent_part(latent_here, segments_here, padded)
    copies[2].wait()
    copies[3].wait()
    scale_part(distances, local, scal, queries_here, exponents_here, outs)


def scale_kernel(distances, local, scal, queries, exponents, *rest):
    outs, (queries_here, exponents_here, sems) = rest[:-3], rest[-3:]
    copies = [
        pltpu.make_async_copy(exponents, exponents_here, sems.at[0]),
        pltpu.make_async_copy(queries, queries_here, sems.at[1]),
    ]
    for copy in copies:
        copy.start()
    for copy in copies:
        copy.wait()
    scale_part(distances, local, scal, queries_here, exponents_here, outs)


def pack_kernel(rows, chips, scal, *refs):
    pieces, (own, upper) = refs[:-2], refs[-2:]
    for slot, piece in enumerate(pieces):
        own[slot * rows : (slot + 1) * rows, :] = piece[...]
    half = chips // 2
    first = jnp.where(scal[0] // 2 < half, half, 0) * rows
    upper[...] = own[pl.ds(pl.multiple_of(first, rows), half * rows), :]


def project_kernel(
    rows, chips, scal, own, earlier, other_own, other_earlier, key_weight, value_weight, keys, values, tail, window
):
    place, core = scal[0] // 2, scal[0] % 2
    lead = chips * rows
    half = chips // 2
    first = jnp.where(place < half, half, 0)
    for slot in range(chips + half):
        if slot < chips:
            to = lead + (place ^ slot) * 2 * rows
            mine, theirs, at = own, other_own, slot * rows
        else:
            to = ((place ^ (first + slot - chips)) - half) * 2 * rows
            mine, theirs, at = earlier, other_earlier, (slot - chips) * rows
        window[pl.ds(pl.multiple_of(to + core * rows, rows), rows), :] = mine[at : at + rows, :]
        window[pl.ds(pl.multiple_of(to + (1 - core) * rows, rows), rows), :] = theirs[at : at + rows, :]
    tail[...] = window[:, LATENT:]
    columns = keys.shape[1]
    tile = min(256, columns)
    step_rows = 256

    def one(step, carry):
        at = pl.multiple_of(step * tile, tile)
        for start in range(0, window.shape[0], step_rows):
            part = window[start : start + step_rows, :LATENT]
            for weight, out in ((key_weight, keys), (value_weight, values)):
                out[start : start + step_rows, pl.ds(at, tile)] = jnp.dot(
                    part, weight[:, pl.ds(at, tile)], preferred_element_type=jnp.float32
                ).astype(jnp.bfloat16)
        return carry

    lax.fori_loop(0, columns // tile, one, 0)


def attend_kernel(rows, chips, local, slot, scal, mine, theirs, keys, values, tail, out_mine, out_theirs):
    place, core = scal[0] // 2, scal[0] % 2
    lead = chips * rows
    chip = place ^ slot
    block = 2 * rows
    width = lead + block
    start = pl.multiple_of(chip * block, block)
    own = pl.multiple_of(lead + start + core * rows, rows)
    other = pl.multiple_of(lead + start + (1 - core) * rows, rows)
    key_tail = tail[pl.ds(start, width), :]
    pick = jnp.where(lax.broadcasted_iota(jnp.int32, (8, LANES), 1) == ROPE, 1.0, 0.0).astype(jnp.bfloat16)
    key_seg = lax.dot_general(pick, key_tail, (((1,), (1,)), ((), ())), preferred_element_type=jnp.float32)[0:1]
    query_tail = jnp.concatenate([tail[pl.ds(own, rows), :], tail[pl.ds(other, rows), :]], axis=0)
    query_seg = query_tail[:, ROPE : ROPE + 1].astype(jnp.float32)
    row = lax.broadcasted_iota(jnp.int32, (block, width), 0)
    column = lax.broadcasted_iota(jnp.int32, (block, width), 1)
    shift = jnp.where(row < rows, core * rows, -core * rows)
    bias = jnp.where((query_seg == key_seg) & (column <= row + shift + lead), 0.0, MINUS)
    lane = lax.broadcasted_iota(jnp.int32, (width, LANES), 1)
    rope_even = jnp.where(lane < ROPE, key_tail.astype(jnp.float32), 0.0)
    rope_odd = pltpu.roll(rope_even, ROPE, 1)
    rope = (rope_even.astype(jnp.bfloat16), rope_odd.astype(jnp.bfloat16))
    factor = math.log2(math.e) / math.sqrt(NOPE + ROPE)
    for head in range(local):
        at = slice(head * LANES, (head + 1) * LANES)
        pair = slice((local + head // 2) * LANES, (local + head // 2 + 1) * LANES)
        query = jnp.concatenate(
            [
                jnp.concatenate([mine[:, at], mine[:, pair]], axis=1),
                jnp.concatenate([theirs[:, at], theirs[:, pair]], axis=1),
            ],
            axis=0,
        )
        key = jnp.concatenate([keys[pl.ds(start, width), at], rope[head % 2]], axis=1)
        scores = lax.dot_general(query, key, (((1,), (1,)), ((), ())), preferred_element_type=jnp.float32)
        scores = scores * factor + bias
        largest = jnp.max(scores, axis=1, keepdims=True)
        weights = jnp.exp2(scores - largest)
        inverse = 1.0 / jnp.sum(weights, axis=1, keepdims=True)
        weighted = jnp.dot(
            weights.astype(jnp.bfloat16), values[pl.ds(start, width), at], preferred_element_type=jnp.float32
        )
        result = (weighted * inverse).astype(jnp.bfloat16)
        out_mine[:, at] = result[:rows]
        out_theirs[:, at] = result[rows:]


def join_kernel(scal, *refs):
    pieces, out = refs[:-1], refs[-1]
    width = pieces[0].shape[1]
    for distance, piece in enumerate(pieces):
        out[:, pl.ds(pl.multiple_of((scal[0] ^ distance) * width, LANES), width)] = piece[...]


def call(kernel, outs, *args, **options):
    return kernel_call(kernel, outs, *args, **options)


def kernel_call(kernel, outs, *args, scratch=(), flops=0, nbytes=0, exps=0, fetched=False):
    vmem = pl.BlockSpec(memory_space=pltpu.VMEM)
    smem = pl.BlockSpec(memory_space=pltpu.SMEM)
    hbm = pl.BlockSpec(memory_space=pltpu.HBM)
    specs = [smem] + [hbm if fetched else vmem] * (len(args) - 1)
    if fetched:
        scratch = [pltpu.VMEM(arg.shape, arg.dtype) for arg in args[1:]]
        scratch.append(pltpu.SemaphoreType.DMA((len(args) - 1,)))
        args = args[:1] + tuple(pltpu.with_memory_space_constraint(arg, pltpu.HBM) for arg in args[1:])
    shapes = [jax.ShapeDtypeStruct(shape, jnp.bfloat16) for shape in outs]
    return pl.pallas_call(
        kernel,
        out_shape=shapes,
        in_specs=specs,
        out_specs=[vmem] * len(outs),
        scratch_shapes=list(scratch),
        cost_estimate=pl.CostEstimate(flops=flops, bytes_accessed=nbytes, transcendentals=exps),
        compiler_params=pltpu.CompilerParams(vmem_limit_bytes=GRANT),
    )(*args)


def layer(queries, exponents, latent, segments, key_weight, value_weight):
    rows = queries.shape[0]
    heads = exponents.shape[1]
    count = lax.axis_size("head")
    blocks = lax.axis_size("blk")
    local = heads // count
    width = queries.shape[1] // count
    chips = count // 2
    lead = chips * rows
    window_rows = 3 * lead
    columns = local * VDIM
    position = lax.axis_index("head").astype(jnp.int32)
    scal = position.reshape(1)

    def swap(block, distance):
        return lax.ppermute(block, "head", [(i, i ^ distance) for i in range(count)])

    far = list(range(chips, count))
    near = list(range(chips))
    piece = (rows, width)
    padded, *far_pieces = call(
        functools.partial(prepare_kernel, far, local),
        [(rows, LATENT + 2 * ROPE)] + [piece] * len(far),
        scal,
        queries,
        exponents,
        latent,
        segments.reshape(1, rows),
        nbytes=2000000,
        fetched=True,
    )
    near_pieces = call(
        functools.partial(scale_kernel, near, local),
        [piece] * len(near),
        scal,
        queries,
        exponents,
        nbytes=2000000,
        fetched=True,
    )
    sent = list(near_pieces) + list(far_pieces)

    half = chips // 2
    pieces = [None] * chips
    pieces[0] = padded
    pieces[half] = swap(padded, chips)
    for k in range(1, half):
        pieces[k] = swap(padded, 2 * k)
    for k in range(1, half):
        pieces[half + k] = swap(pieces[half], 2 * k)
    row_width = LATENT + 2 * ROPE
    own, upper = call(
        functools.partial(pack_kernel, rows, chips),
        [(lead, row_width), (half * rows, row_width)],
        scal,
        *pieces,
        nbytes=400000,
    )
    other_own = swap(own, 1)
    earlier = lax.ppermute(upper, "blk", [(i, i + 1) for i in range(blocks - 1)])
    other_earlier = swap(earlier, 1)

    arrived = [sent[0]] + [swap(sent[distance], distance) for distance in range(1, count)]

    keys, values, tail = call(
        functools.partial(project_kernel, rows, chips),
        [(window_rows, columns), (window_rows, columns), (window_rows, LANES)],
        scal,
        own,
        earlier,
        other_own,
        other_earlier,
        key_weight,
        value_weight,
        scratch=[pltpu.VMEM((window_rows, LATENT + LANES), jnp.bfloat16)],
        flops=4 * window_rows * LATENT * columns,
        nbytes=4 * LATENT * columns,
    )

    returned = [None] * count
    span = lead + 2 * rows
    for slot in range(chips):
        results = call(
            functools.partial(attend_kernel, rows, chips, local, slot),
            [(rows, columns)] * 2,
            scal,
            arrived[2 * slot],
            arrived[2 * slot + 1],
            keys,
            values,
            tail,
            flops=2 * 2 * rows * span * local * 384,
            nbytes=4 * rows * (width + columns),
            exps=2 * rows * span * local,
        )
        for distance, result in zip((2 * slot, 2 * slot + 1), results):
            returned[distance] = result if distance == 0 else swap(result, distance)
    (joined,) = call(join_kernel, [(rows, heads * VDIM)], scal, *returned, nbytes=4 * rows * heads * VDIM)
    return joined


def solution(mesh):
    in_specs = (
        P(("blk", "head"), None),
        P(("blk", "head"), None),
        P(("blk", "head"), None),
        P(("blk", "head")),
        P(None, "head"),
        P(None, "head"),
    )
    out_specs = P(("blk", "head"), None)
    return jax.shard_map(layer, mesh=mesh, in_specs=in_specs, out_specs=out_specs, check_vma=False)
```
